32 devices in a mesh: seq: 8 (over z, y), fsdp: 4 (over x, core).
Axes of the slice: x: 2, y: 2, z: 4, core: 2. Of those that a mesh axis runs over, the one named last changes fastest.
Arguments:
- queries: bfloat16 [1024, 2048], P('seq', 'fsdp'), may hold values from -260 to 260
- layer_input: bfloat16 [1024, 4096], P('seq'), may hold values from -6 to 6
- w_key: bfloat16 [4096, 512], P('seq', 'fsdp'), may hold values from -0.09375 to 0.09375
- w_value: bfloat16 [4096, 512], P('seq', 'fsdp'), may hold values from -0.09375 to 0.09375
- grad_out: bfloat16 [1024, 2048], P('seq', 'fsdp'), may hold values from -6 to 6
Outputs:
- attn_out: bfloat16 [1024, 2048], P('seq', 'fsdp')
- grad_queries: bfloat16 [1024, 2048], P('seq', 'fsdp')
- grad_input: bfloat16 [1024, 4096], P('seq', 'fsdp')
- grad_w_key: float32 [4096, 512], P('seq', 'fsdp')
- grad_w_value: float32 [4096, 512], P('seq', 'fsdp')
The draws below stay inside these ranges and needn't reach their ends.
All inputs are finite; a program needn't handle non-finite values.
Results may differ from the reference program's by a relative error of at most 0.04.
Values may be sent and summed in bfloat16 or wider, within the bound.
A program may use at most 64 MiB of HBM per device.

```python
import math
import jax
import jax.numpy as jnp
from jax import lax

D = 4096
HD = 128
KV_HEADS = 4
GROUP = 4
QW = 2048
KVW = 512
TOKENS = 1024


def draw_queries(key, part):
    base = jnp.clip(jax.random.normal(key, (TOKENS, QW), jnp.float32), -6.0, 6.0)
    return base.astype(jnp.bfloat16)


def level_of(rng, dims, pieces, smallest, top_value):
    factor_of = 1.0
    for axis_at, shards_of in pieces:
        heights = jax.random.uniform(jax.random.fold_in(jax.random.fold_in(rng, 6), axis_at), (shards_of,), jnp.float32, smallest / len(pieces), top_value / len(pieces))
        factor_of = factor_of * jnp.repeat(jnp.exp(heights), dims[axis_at] // shards_of).reshape((-1,) + (1,) * (len(dims) - 1 - axis_at))
    return factor_of


def scatter_about(own_key, shape, deviation, limit, pieces=(), kind=jnp.bfloat16):
    result = jax.random.normal(own_key, shape, jnp.float32) * deviation
    if len(pieces) > 0:
        result = level_of(own_key, shape, pieces, -0.22, 0.18) * result
    return jnp.clip(result, min=-limit, max=limit).astype(kind)


def setup_inputs(seed: int = 0) -> dict:
    arg_keys = jax.random.split(jax.random.key(seed), 6)
    return {
        "queries": draw_queries(jax.random.fold_in(arg_keys[5], 71), 0),
        "layer_input": scatter_about(arg_keys[1], (TOKENS, D), 1.0, 6.0, ((0, 8),)),
        "w_key": scatter_about(arg_keys[2], (D, KVW), D ** -0.5, 0.09375, ((0, 8), (1, 4))),
        "w_value": scatter_about(arg_keys[3], (D, KVW), D ** -0.5, 0.09375, ((0, 8), (1, 4))),
        "grad_out": scatter_about(arg_keys[4], (TOKENS, QW), 1.0, 6.0, ((0, 8), (1, 4))),
    }


ROPE_BASE = 500000.0
NEG = -1.0e30


def rope_tables(positions, half):
    freq = ROPE_BASE ** (-(jnp.arange(half, dtype=jnp.float32) * (2.0 / (2 * half))))
    angle = positions.astype(jnp.float32)[:, None] * freq[None, :]
    return jnp.cos(angle), jnp.sin(angle)


def rotate(heads, cosine, sine):
    half = heads.shape[-1] // 2
    first = heads[..., :half]
    second = heads[..., half:]
    cos_b = cosine[:, None, :]
    sin_b = sine[:, None, :]
    return jnp.concatenate([first * cos_b - second * sin_b, second * cos_b + first * sin_b], axis=-1)


def to_low(array):
    return lax.optimization_barrier(array.astype(jnp.bfloat16)).astype(jnp.float32)


def reference(queries, layer_input, w_key, w_value, grad_out):
    scale = HD ** -0.5
    key_linear = jnp.dot(layer_input, w_key, preferred_element_type=jnp.float32).reshape(TOKENS, KV_HEADS, HD)
    value_rows = jnp.dot(layer_input, w_value, preferred_element_type=jnp.float32).astype(jnp.bfloat16)
    value_rows = value_rows.reshape(TOKENS, KV_HEADS, HD)
    positions = jnp.arange(TOKENS, dtype=jnp.int32)
    cosine, sine = rope_tables(positions, HD // 2)
    keys = rotate(key_linear, cosine, sine).astype(jnp.bfloat16)
    keys_wide = keys.astype(jnp.float32)
    values_wide = value_rows.astype(jnp.float32)
    query = queries.astype(jnp.float32).reshape(TOKENS, KV_HEADS, GROUP, HD)
    upstream = grad_out.astype(jnp.float32).reshape(TOKENS, KV_HEADS, GROUP, HD)
    block = math.gcd(TOKENS, 256)
    count = TOKENS // block
    key_pos = jnp.arange(TOKENS, dtype=jnp.int32)

    def block_scores(index):
        start = (index * block).astype(jnp.int32)
        rows = lax.dynamic_slice_in_dim(query, start, block, 0)
        scores = jnp.einsum("qhgd,khd->hgqk", rows, keys_wide) * scale
        query_pos = start + jnp.arange(block, dtype=jnp.int32)
        mask = key_pos[None, :] <= query_pos[:, None]
        return rows, jnp.where(mask, scores, NEG), mask

    def forward_block(index):
        rows, scores, mask = block_scores(index)
        top = jnp.max(scores, axis=-1, keepdims=True)
        total = jnp.sum(jnp.where(mask, jnp.exp(scores - top), 0.0), axis=-1, keepdims=True)
        lse = top + jnp.log(total)
        probs = to_low(jnp.where(mask, jnp.exp(scores - lse), 0.0))
        return jnp.einsum("hgqk,khd->qhgd", probs, values_wide), lse[..., 0]

    outs, lses = lax.map(forward_block, jnp.arange(count, dtype=jnp.int32))
    output = outs.reshape(TOKENS, KV_HEADS, GROUP, HD)
    lse_all = jnp.transpose(lses, (1, 2, 0, 3)).reshape(KV_HEADS, GROUP, TOKENS)
    delta_all = jnp.transpose(jnp.sum(upstream * output, axis=-1), (1, 2, 0))

    def backward_block(carry, index):
        key_acc, value_acc = carry
        rows, scores, mask = block_scores(index)
        start = (index * block).astype(jnp.int32)
        lse_blk = lax.dynamic_slice_in_dim(lse_all, start, block, 2)
        delta_blk = lax.dynamic_slice_in_dim(delta_all, start, block, 2)
        up_rows = lax.dynamic_slice_in_dim(upstream, start, block, 0)
        probs = jnp.where(mask, jnp.exp(scores - lse_blk[..., None]), 0.0)
        dprobs = jnp.einsum("qhgd,khd->hgqk", up_rows, values_wide)
        dscores = probs * (dprobs - delta_blk[..., None])
        value_acc = value_acc + jnp.einsum("hgqk,qhgd->khd", to_low(probs), up_rows)
        ds_low = to_low(dscores)
        query_grad = jnp.einsum("hgqk,khd->qhgd", ds_low, keys_wide) * scale
        key_acc = key_acc + jnp.einsum("hgqk,qhgd->khd", ds_low, rows) * scale
        return (key_acc, value_acc), query_grad.astype(jnp.bfloat16)

    zeros = jnp.zeros((TOKENS, KV_HEADS, HD), jnp.float32)
    (key_acc, value_acc), query_grads = lax.scan(backward_block, (zeros, zeros), jnp.arange(count, dtype=jnp.int32))
    key_grad = rotate(key_acc, cosine, -sine).astype(jnp.bfloat16).reshape(TOKENS, KVW)
    value_grad = value_acc.astype(jnp.bfloat16).reshape(TOKENS, KVW)
    grad_w_key = jnp.dot(layer_input.T, key_grad, preferred_element_type=jnp.float32)
    grad_w_value = jnp.dot(layer_input.T, value_grad, preferred_element_type=jnp.float32)
    grad_input = (jnp.dot(key_grad, w_key.T, preferred_element_type=jnp.float32)
                  + jnp.dot(value_grad, w_value.T, preferred_element_type=jnp.float32)).astype(jnp.bfloat16)
    attn_out = output.reshape(TOKENS, QW).astype(jnp.bfloat16)
    return attn_out, query_grads.reshape(TOKENS, QW), grad_input, grad_w_key, grad_w_value
```

```python
import functools

import jax
import jax.numpy as jnp
import numpy as np
from jax import lax
from jax.experimental import pallas as pl
from jax.experimental.pallas import tpu as pltpu
from jax.sharding import PartitionSpec as P

HD = 128
ROPE_BASE = 500000.0
NEG = -1e30
MESH = pl.DeviceIdType.MESH
F32 = jnp.float32
BF16 = jnp.bfloat16


def loop(low, high, step):
    def run(i, carry):
        step(i)
        return carry

    lax.fori_loop(low, high, run, 0)


def dot_nn(a, b):
    return lax.dot_general(a, b, (((1,), (0,)), ((), ())), preferred_element_type=F32)


def dot_nt(a, b):
    return lax.dot_general(a, b, (((1,), (1,)), ((), ())), preferred_element_type=F32)


def dot_tn(a, b):
    return lax.dot_general(a, b, (((0,), (0,)), ((), ())), preferred_element_type=F32)


def kernel(cfg, *refs):
    n, nf, exchange = cfg
    q_ref, x_ref, wk_ref, wv_ref, g_ref, freq_ref = refs[:6]
    refs = refs[6:]
    if not exchange:
        xt_in = refs[0]
        refs = refs[1:]
    ao_ref, gq_ref, gi_ref, gwk_ref, gwv_ref = refs[:5]
    (wk_all, wv_all, kv_all, dkv_all, xt, q_st, g_st, o_acc, dq_acc, m_acc, l_acc, s_scr,
     rs_send, rs_recv, own_dkv, cos_scr, sin_scr, gi_send, gi_recv, gi_own,
     wk_s, wk_r, wv_s, wv_r, kv_s, kv_r, dkv_s, dkv_r, x_s, x_r, xf_s, xf_r,
     rs_s, rs_r, gi_s, gi_r) = refs[5:]
    tok = x_ref.shape[0]
    rows, cols = wk_ref.shape
    heads = cols // HD
    group = q_ref.shape[1] // cols
    m_rows = group * tok
    part = rows // nf
    width = gi_ref.shape[1]
    scale = HD ** (-0.5)
    s = lax.axis_index("seq")
    f = lax.axis_index("fsdp")
    inner = 2 if n % 2 == 0 else 1
    outer = n // inner
    z = s // inner
    y = s % inner
    mate = z * inner + (inner - 1 - y)

    def copy(src, dst, send, recv, dev):
        return pltpu.make_async_remote_copy(
            src_ref=src, dst_ref=dst, send_sem=send, recv_sem=recv, device_id=dev,
            device_id_type=MESH,
        )

    barrier = pltpu.get_barrier_semaphore()

    def greet_seq(d):
        pl.semaphore_signal(
            barrier, inc=1, device_id=((s + d) % n, f), device_id_type=MESH)

    def greet_fsdp(d):
        pl.semaphore_signal(
            barrier, inc=1, device_id=(s, (f + d) % nf), device_id_type=MESH)

    loop(1, n, greet_seq)
    loop(1, nf, greet_fsdp)
    pl.semaphore_wait(barrier, n + nf - 2)

    class Gather:
        def __init__(self, own, slot, send, recv):
            self.own, self.slot, self.send, self.recv = own, slot, send, recv

        def outgoing(self, d):
            return copy(self.own, self.slot(s), self.send.at[d], self.recv.at[s],
                        ((z + d) % outer * inner + y, f))

        def to_mate(self):
            return copy(self.own, self.slot(s), self.send.at[0], self.recv.at[s], (mate, f))

        def arrived(self, b):
            copy(self.own, self.slot(b), self.send.at[0], self.recv.at[b], (mate, f)).wait_recv()

        def pass_on(self, d):
            b = (z - d + outer) % outer * inner + y
            return copy(self.slot(b), self.slot(b), self.send.at[outer + d], self.recv.at[b],
                        (mate, f))

        def start(self):
            if inner == 2:
                self.to_mate().start()
            loop(1, outer, lambda d: self.outgoing(d).start())

        def forward(self):
            def step(d):
                self.arrived((z - d + outer) % outer * inner + y)
                if inner == 2:
                    self.pass_on(d).start()

            loop(1, outer, step)

        def finish(self):
            if inner == 2:
                loop(0, outer, lambda d: self.arrived(
                    (z - d + outer) % outer * inner + (inner - 1 - y)))

        def drain(self):
            if inner == 2:
                self.to_mate().wait_send()
            loop(1, outer, lambda d: self.outgoing(d).wait_send())
            if inner == 2:
                loop(1, outer, lambda d: self.pass_on(d).wait_send())

    def row_slot(ref, size):
        return lambda b: ref.at[pl.ds(pl.multiple_of(b * size, size), size)]

    wk_gather = Gather(wk_ref, row_slot(wk_all, rows), wk_s, wk_r)
    wv_gather = Gather(wv_ref, row_slot(wv_all, rows), wv_s, wv_r)
    kv_slot = row_slot(kv_all, tok)
    kv_gather = Gather(kv_slot(s), kv_slot, kv_s, kv_r)
    dkv_slot = row_slot(dkv_all, tok)
    dkv_gather = Gather(dkv_slot(s), dkv_slot, dkv_s, dkv_r)

    wk_gather.start()
    wv_gather.start()

    if exchange:
        def x_src(b):
            return x_ref.at[:, pl.ds(pl.multiple_of(b * rows + f * part, part), part)]

        def x_copy(d):
            b = (s + d) % n
            return copy(x_src(b), xt.at[f, pl.ds(pl.multiple_of(s * tok, tok), tok)],
                        x_s.at[d], x_r.at[s], (b, f))

        def x_arrived(d):
            b = (s + d) % n
            copy(x_src(b), xt.at[f, pl.ds(pl.multiple_of(b * tok, tok), tok)],
                 x_s.at[d], x_r.at[b], (b, f)).wait_recv()

        def xf_copy(d):
            return copy(xt.at[f], xt.at[f], xf_s.at[d], xf_r.at[f], (s, (f + d) % nf))

        def xf_arrived(d):
            b = (f + d) % nf
            copy(xt.at[f], xt.at[b], xf_s.at[d], xf_r.at[b], (s, b)).wait_recv()

        loop(1, n, lambda d: x_copy(d).start())
        xt[f, pl.ds(pl.multiple_of(s * tok, tok), tok), :] = x_ref[
            :, pl.ds(pl.multiple_of(s * rows + f * part, part), part)]

    wk_all[pl.ds(pl.multiple_of(s * rows, rows), rows), :] = wk_ref[...]
    wv_all[pl.ds(pl.multiple_of(s * rows, rows), rows), :] = wv_ref[...]
    for h in range(heads):
        for g in range(group):
            c = (h * group + g) * HD
            q_st[h, g * tok:(g + 1) * tok, :] = q_ref[:, c:c + HD]
            g_st[h, g * tok:(g + 1) * tok, :] = g_ref[:, c:c + HD]
    lane = lax.broadcasted_iota(jnp.int32, (tok, HD), 1)
    position = (s * tok + lax.broadcasted_iota(jnp.int32, (tok, HD), 0)).astype(F32)
    angle = position * freq_ref[...]
    cos_scr[...] = jnp.cos(angle)
    sin_scr[...] = jnp.where(lane < HD // 2, -jnp.sin(angle), jnp.sin(angle))

    wk_gather.forward()
    wv_gather.forward()
    wk_gather.finish()
    wv_gather.finish()

    key_lin = dot_nn(x_ref[...], wk_all[...])
    value_lin = dot_nn(x_ref[...], wv_all[...])
    own_rows = pl.ds(pl.multiple_of(s * tok, tok), tok)
    for h in range(heads):
        lin = key_lin[:, h * HD:(h + 1) * HD]
        turned = lin * cos_scr[...] + pltpu.roll(lin, HD // 2, 1) * sin_scr[...]
        kv_all[own_rows, h * HD:(h + 1) * HD] = turned.astype(BF16)
    kv_all[own_rows, cols:] = value_lin.astype(BF16)
    kv_gather.start()

    if exchange:
        loop(1, n, x_arrived)
        loop(1, nf, lambda d: xf_copy(d).start())

    kv_gather.forward()
    kv_gather.finish()

    def key_of(j, h):
        return kv_all[pl.ds(pl.multiple_of(j * tok, tok), tok), h * HD:(h + 1) * HD]

    def value_of(j, h):
        return kv_all[pl.ds(pl.multiple_of(j * tok, tok), tok), cols + h * HD:cols + (h + 1) * HD]

    deltas, inverses = [], []
    for h in range(heads):
        m_acc[...] = jnp.full(m_acc.shape, NEG, F32)
        l_acc[...] = jnp.zeros(l_acc.shape, F32)
        o_acc[...] = jnp.zeros(o_acc.shape, F32)

        def score(j):
            sc = dot_nt(q_st[h], key_of(j, h)) * scale
            row = lax.broadcasted_iota(jnp.int32, (m_rows, tok), 0) % tok
            col = lax.broadcasted_iota(jnp.int32, (m_rows, tok), 1)
            sc = jnp.where(col + j * tok <= row + s * tok, sc, NEG)
            s_scr[h * n + j] = sc
            m_acc[...] = jnp.maximum(m_acc[...], sc)

        loop(0, s + 1, score)
        top = jnp.max(m_acc[...], axis=1, keepdims=True)

        def weigh(j):
            e = jnp.exp(s_scr[h * n + j] - top)
            s_scr[h * n + j] = e
            l_acc[...] += e
            o_acc[...] += dot_nn(e.astype(BF16), value_of(j, h))

        loop(0, s + 1, weigh)
        inverse = 1.0 / jnp.sum(l_acc[...], axis=1, keepdims=True)
        out = o_acc[...] * inverse
        delta = jnp.sum(g_st[h].astype(F32) * out, axis=1, keepdims=True)
        for g in range(group):
            c = (h * group + g) * HD
            ao_ref[:, c:c + HD] = out[g * tok:(g + 1) * tok].astype(BF16)
        deltas.append(delta)
        inverses.append(inverse)

    dq_acc[...] = jnp.zeros(dq_acc.shape, F32)

    def backward(j, h):
        p = s_scr[h * n + j] * inverses[h]
        dp = dot_nt(g_st[h], value_of(j, h))
        ds = (p * (dp - deltas[h])).astype(BF16)
        dv = dot_tn(p.astype(BF16), g_st[h])
        dk = dot_tn(ds, q_st[h])
        dq_acc[h] += dot_nn(ds, key_of(j, h))
        return dk, dv

    def rs_copy(j):
        return copy(rs_send.at[j], rs_recv.at[s], rs_s.at[j], rs_r.at[s], (j, f))

    def give(j):
        for h in range(heads):
            dk, dv = backward(j, h)
            rs_send[j, :, h * HD:(h + 1) * HD] = dk.astype(BF16)
            rs_send[j, :, cols + h * HD:cols + (h + 1) * HD] = dv.astype(BF16)
        rs_copy(j).start()

    loop(0, s, give)
    for h in range(heads):
        dk, dv = backward(s, h)
        own_dkv[:, h * HD:(h + 1) * HD] = dk
        own_dkv[:, cols + h * HD:cols + (h + 1) * HD] = dv
        for g in range(group):
            c = (h * group + g) * HD
            gq_ref[:, c:c + HD] = (dq_acc[h, g * tok:(g + 1) * tok] * scale).astype(BF16)

    def take(j):
        copy(rs_send.at[0], rs_recv.at[j], rs_s.at[0], rs_r.at[j], (mate, f)).wait_recv()
        own_dkv[...] += rs_recv[j].astype(F32)

    loop(s + 1, n, take)
    for h in range(heads):
        lin = own_dkv[:, h * HD:(h + 1) * HD] * scale
        turned = lin * cos_scr[...] - pltpu.roll(lin, HD // 2, 1) * sin_scr[...]
        dkv_all[own_rows, h * HD:(h + 1) * HD] = turned.astype(BF16)
    dkv_all[own_rows, cols:] = own_dkv[:, cols:].astype(BF16)
    dkv_gather.start()

    def input_term(b):
        at = pl.ds(pl.multiple_of(b * width, width), width)
        return (dot_nt(dkv_all[own_rows, :cols], wk_all[at, :])
                + dot_nt(dkv_all[own_rows, cols:], wv_all[at, :]))

    def gi_copy(d):
        return copy(gi_send.at[d], gi_recv.at[f], gi_s.at[d], gi_r.at[f], (s, (f + d) % nf))

    def gi_give(d):
        gi_send[d] = input_term((f + d) % nf).astype(BF16)
        gi_copy(d).start()

    loop(1, nf, gi_give)
    gi_own[...] = input_term(f)
    if exchange:
        loop(1, nf, xf_arrived)
    dkv_gather.forward()
    dkv_gather.finish()

    total_tok = n * tok
    step = min(total_tok, 1024)
    for i in range(nf if exchange else 1):
        grad = None
        for at in range(0, total_tok, step):
            left = xt[i, at:at + step, :] if exchange else xt_in[at:at + step, :]
            term = dot_tn(left, dkv_all[at:at + step, :])
            grad = term if grad is None else grad + term
        count = grad.shape[0]
        gwk_ref[i * count:(i + 1) * count, :] = grad[:, :cols]
        gwv_ref[i * count:(i + 1) * count, :] = grad[:, cols:]

    def gi_take(d):
        b = (f + d) % nf
        copy(gi_send.at[d], gi_recv.at[b], gi_s.at[d], gi_r.at[b], (s, b)).wait_recv()
        gi_own[...] += gi_recv[b].astype(F32)

    loop(1, nf, gi_take)
    gi_ref[...] = gi_own[...].astype(BF16)

    for gather in (wk_gather, wv_gather, kv_gather, dkv_gather):
        gather.drain()
    if exchange:
        loop(1, n, lambda d: x_copy(d).wait_send())
        loop(1, nf, lambda d: xf_copy(d).wait_send())
    loop(0, s, lambda j: rs_copy(j).wait_send())
    loop(1, nf, lambda d: gi_copy(d).wait_send())


def body(n, nf, queries, layer_input, w_key, w_value, grad_out):
    tok, depth = layer_input.shape
    rows, cols = w_key.shape
    heads = cols // HD
    group = queries.shape[1] // cols
    m_rows = group * tok
    part = rows // nf
    exchange = part % 128 == 0
    half = HD // 2
    freq = np.float32(ROPE_BASE) ** (-(np.arange(half, dtype=np.float32) * np.float32(2.0 / HD)))
    freq = jnp.asarray(np.concatenate([freq, freq])[None, :], F32)
    operands = [queries, layer_input, w_key, w_value, grad_out, freq]
    if not exchange:
        operands.append(
            lax.all_to_all(layer_input, "seq", split_axis=1, concat_axis=0, tiled=True))
    width = depth // nf
    x_rows = n * tok if exchange else 16
    x_cols = part if exchange else 128
    vmem = pltpu.VMEM
    dma = pltpu.SemaphoreType.DMA
    scratch = [
        vmem((depth, cols), BF16), vmem((depth, cols), BF16),
        vmem((n * tok, 2 * cols), BF16), vmem((n * tok, 2 * cols), BF16),
        vmem((nf, x_rows, x_cols), BF16),
        vmem((heads, m_rows, HD), BF16), vmem((heads, m_rows, HD), BF16),
        vmem((m_rows, HD), F32), vmem((heads, m_rows, HD), F32),
        vmem((m_rows, tok), F32), vmem((m_rows, tok), F32),
        vmem((heads * n, m_rows, tok), F32),
        vmem((n, tok, 2 * cols), BF16), vmem((n, tok, 2 * cols), BF16),
        vmem((tok, 2 * cols), F32),
        vmem((tok, HD), F32), vmem((tok, HD), F32),
        vmem((nf, tok, width), BF16), vmem((nf, tok, width), BF16), vmem((tok, width), F32),
    ]
    for _ in range(4):
        scratch += [dma((2 * n,)), dma((n,))]
    scratch += [dma((n,)), dma((n,)), dma((nf,)), dma((nf,))]
    scratch += [dma((n,)), dma((n,)), dma((nf,)), dma((nf,))]
    out_shape = [
        jax.ShapeDtypeStruct(queries.shape, BF16),
        jax.ShapeDtypeStruct(queries.shape, BF16),
        jax.ShapeDtypeStruct((tok, width), BF16),
        jax.ShapeDtypeStruct((rows, cols), F32),
        jax.ShapeDtypeStruct((rows, cols), F32),
    ]
    spec = pl.BlockSpec(memory_space=pltpu.VMEM)
    return tuple(pl.pallas_call(
        functools.partial(kernel, (n, nf, exchange)),
        out_shape=out_shape,
        in_specs=[spec] * len(operands),
        out_specs=[spec] * len(out_shape),
        scratch_shapes=scratch,
        compiler_params=pltpu.CompilerParams(
            collective_id=0, has_side_effects=True, vmem_limit_bytes=60 * 1024 * 1024),
    )(*operands))


def solution(mesh):
    placed = (
        P("seq", "fsdp"),
        P("seq", None),
        P("seq", "fsdp"),
        P("seq", "fsdp"),
        P("seq", "fsdp"),
    )
    return jax.shard_map(
        functools.partial(body, mesh.shape["seq"], mesh.shape["fsdp"]),
        mesh=mesh,
        in_specs=placed,
        out_specs=(P("seq", "fsdp"),) * 5,
        check_vma=False,
    )
```

```python
import functools

import jax
import jax.numpy as jnp
import numpy as np
from jax import lax
from jax.experimental import pallas as pl
from jax.experimental.pallas import tpu as pltpu
from jax.sharding import PartitionSpec as P

HD = 128
ROPE_BASE = 500000.0
NEG = -1e30
MESH = pl.DeviceIdType.MESH
F32 = jnp.float32
BF16 = jnp.bfloat16


def loop(low, high, step):
    def run(i, carry):
        step(i)
        return carry

    lax.fori_loop(low, high, run, 0)


def dot_nn(a, b):
    return lax.dot_general(a, b, (((1,), (0,)), ((), ())), preferred_element_type=F32)


def dot_nt(a, b):
    return lax.dot_general(a, b, (((1,), (1,)), ((), ())), preferred_element_type=F32)


def dot_tn(a, b):
    return lax.dot_general(a, b, (((0,), (0,)), ((), ())), preferred_element_type=F32)


def kernel(cfg, *refs):
    n, nf, exchange = cfg
    q_hbm, x_hbm, wk_ref, wv_ref, g_hbm, freq_ref = refs[:6]
    refs = refs[6:]
    if not exchange:
        xt_in = refs[0]
        refs = refs[1:]
    ao_ref, gq_ref, gi_ref, gwk_ref, gwv_ref = refs[:5]
    (wk_all, wv_all, kv_all, dkv_all, xt, q_st, g_st, o_acc, dq_acc, m_acc, l_acc, s_scr,
     rs_send, rs_recv, own_dkv, cos_scr, sin_scr, gi_send, gi_recv, gi_own,
     wk_s, wk_r, wv_s, wv_r, kv_s, kv_r, dkv_s, dkv_r, x_s, x_r, xf_s, xf_r,
     rs_s, rs_r, gi_s, gi_r, q_ref, x_ref, g_ref, in_s) = refs[5:]
    tok = x_ref.shape[0]
    rows, cols = wk_ref.shape
    heads = cols // HD
    group = q_ref.shape[1] // cols
    m_rows = group * tok
    part = rows // nf
    width = gi_ref.shape[1]
    scale = HD ** (-0.5)
    s = lax.axis_index("seq")
    f = lax.axis_index("fsdp")
    inner = 2 if n % 2 == 0 else 1
    outer = n // inner
    z = s // inner
    y = s % inner
    mate = z * inner + (inner - 1 - y)

    def copy(src, dst, send, recv, dev):
        return pltpu.make_async_remote_copy(
            src_ref=src, dst_ref=dst, send_sem=send, recv_sem=recv, device_id=dev,
            device_id_type=MESH,
        )

    barrier = pltpu.get_barrier_semaphore()

    def greet_seq(d):
        pl.semaphore_signal(
            barrier, inc=1, device_id=((s + d) % n, f), device_id_type=MESH)

    def greet_fsdp(d):
        pl.semaphore_signal(
            barrier, inc=1, device_id=(s, (f + d) % nf), device_id_type=MESH)

    loop(1, n, greet_seq)
    loop(1, nf, greet_fsdp)
    mine = pl.ds(pl.multiple_of(s * rows, rows), rows)
    loads = [
        pltpu.make_async_copy(src, dst, in_s.at[i])
        for i, (src, dst) in enumerate((
            (wk_ref, wk_all.at[mine]), (wv_ref, wv_all.at[mine]),
            (x_hbm, x_ref), (q_hbm, q_ref), (g_hbm, g_ref)))
    ]
    for load in loads:
        load.start()
    pl.semaphore_wait(barrier, n + nf - 2)

    class Gather:
        def __init__(self, own, slot, send, recv):
            self.own, self.slot, self.send, self.recv = own, slot, send, recv

        def outgoing(self, d):
            return copy(self.own, self.slot(s), self.send.at[d], self.recv.at[s],
                        ((z + d) % outer * inner + y, f))

        def to_mate(self):
            return copy(self.own, self.slot(s), self.send.at[0], self.recv.at[s], (mate, f))

        def arrived(self, b):
            copy(self.own, self.slot(b), self.send.at[0], self.recv.at[b], (mate, f)).wait_recv()

        def pass_on(self, d):
            b = (z - d + outer) % outer * inner + y
            return copy(self.slot(b), self.slot(b), self.send.at[outer + d], self.recv.at[b],
                        (mate, f))

        def start(self):
            if inner == 2:
                self.to_mate().start()
            loop(1, outer, lambda d: self.outgoing(d).start())

        def forward(self):
            def step(d):
                self.arrived((z - d + outer) % outer * inner + y)
                if inner == 2:
                    self.pass_on(d).start()

            loop(1, outer, step)

        def finish(self):
            if inner == 2:
                loop(0, outer, lambda d: self.arrived(
                    (z - d + outer) % outer * inner + (inner - 1 - y)))

        def drain(self):
            if inner == 2:
                self.to_mate().wait_send()
            loop(1, outer, lambda d: self.outgoing(d).wait_send())
            if inner == 2:
                loop(1, outer, lambda d: self.pass_on(d).wait_send())

    class Line(Gather):
        def hop(self, b, way):
            ref = self.slot(b)
            dev = (z + 1) * inner + y if way == 0 else (z - 1) * inner + y if way == 1 else mate
            return copy(ref, ref, self.send.at[way * n + b], self.recv.at[b], (dev, f))

        def first(self, way):
            dev = (z + 1) * inner + y if way == 0 else (z - 1) * inner + y if way == 1 else mate
            return copy(self.own, self.slot(s), self.send.at[way * n + s], self.recv.at[s],
                        (dev, f))

        def start(self):
            pl.when(z < outer - 1)(lambda: self.first(0).start())
            pl.when(z > 0)(lambda: self.first(1).start())
            if inner == 2:
                self.first(2).start()

        def relay(self, d, act):
            below = (z - d) * inner + y
            above = (z + d) * inner + y

            @pl.when(z >= d)
            def _():
                if act == "start":
                    self.arrived(below)
                for way in (0, 2) if inner == 2 else (0,):
                    def go(way=way):
                        getattr(self.hop(below, way), act)()
                    if way == 0:
                        pl.when(z < outer - 1)(go)
                    else:
                        go()

            @pl.when(z + d < outer)
            def _():
                if act == "start":
                    self.arrived(above)
                for way in (1, 2) if inner == 2 else (1,):
                    def go(way=way):
                        getattr(self.hop(above, way), act)()
                    if way == 1:
                        pl.when(z > 0)(go)
                    else:
                        go()

        def drain(self):
            pl.when(z < outer - 1)(lambda: self.first(0).wait_send())
            pl.when(z > 0)(lambda: self.first(1).wait_send())
            if inner == 2:
                self.first(2).wait_send()
            loop(1, outer, lambda d: self.relay(d, "wait_send"))

    def row_slot(ref, size):
        return lambda b: ref.at[pl.ds(pl.multiple_of(b * size, size), size)]

    wk_slot, wv_slot = row_slot(wk_all, rows), row_slot(wv_all, rows)
    wk_gather = Line(wk_slot(s), wk_slot, wk_s, wk_r)
    wv_gather = Line(wv_slot(s), wv_slot, wv_s, wv_r)
    kv_slot = row_slot(kv_all, tok)
    kv_gather = Gather(kv_slot(s), kv_slot, kv_s, kv_r)
    dkv_slot = row_slot(dkv_all, tok)
    dkv_gather = Gather(dkv_slot(s), dkv_slot, dkv_s, dkv_r)

    loads[0].wait()
    wk_gather.start()
    loads[1].wait()
    wv_gather.start()
    for load in loads[2:]:
        load.wait()

    if exchange:
        def x_src(b):
            return x_ref.at[:, pl.ds(pl.multiple_of(b * rows + f * part, part), part)]

        def x_copy(d):
            b = (s + d) % n
            return copy(x_src(b), xt.at[f, pl.ds(pl.multiple_of(s * tok, tok), tok)],
                        x_s.at[d], x_r.at[s], (b, f))

        def x_arrived(d):
            b = (s + d) % n
            copy(x_src(b), xt.at[f, pl.ds(pl.multiple_of(b * tok, tok), tok)],
                 x_s.at[d], x_r.at[b], (b, f)).wait_recv()

        def xf_copy(d):
            return copy(xt.at[f], xt.at[f], xf_s.at[d], xf_r.at[f], (s, (f + d) % nf))

        def xf_arrived(d):
            b = (f + d) % nf
            copy(xt.at[f], xt.at[b], xf_s.at[d], xf_r.at[b], (s, b)).wait_recv()

        xt[f, pl.ds(pl.multiple_of(s * tok, tok), tok), :] = x_ref[
            :, pl.ds(pl.multiple_of(s * rows + f * part, part), part)]

    for h in range(heads):
        for g in range(group):
            c = (h * group + g) * HD
            q_st[h, g * tok:(g + 1) * tok, :] = q_ref[:, c:c + HD]
            g_st[h, g * tok:(g + 1) * tok, :] = g_ref[:, c:c + HD]
    lane = lax.broadcasted_iota(jnp.int32, (tok, HD), 1)
    position = (s * tok + lax.broadcasted_iota(jnp.int32, (tok, HD), 0)).astype(F32)
    angle = position * freq_ref[...]
    cos_scr[...] = jnp.cos(angle)
    sin_scr[...] = jnp.where(lane < HD // 2, -jnp.sin(angle), jnp.sin(angle))

    def relay_weights(d):
        wk_gather.relay(d, "start")
        wv_gather.relay(d, "start")

    loop(1, outer, relay_weights)
    wk_gather.finish()
    wv_gather.finish()

    key_lin = dot_nn(x_ref[...], wk_all[...])
    value_lin = dot_nn(x_ref[...], wv_all[...])
    own_rows = pl.ds(pl.multiple_of(s * tok, tok), tok)
    for h in range(heads):
        lin = key_lin[:, h * HD:(h + 1) * HD]
        turned = lin * cos_scr[...] + pltpu.roll(lin, HD // 2, 1) * sin_scr[...]
        kv_all[own_rows, h * HD:(h + 1) * HD] = turned.astype(BF16)
    kv_all[own_rows, cols:] = value_lin.astype(BF16)
    kv_gather.start()

    if exchange:
        loop(1, n, lambda d: x_copy(d).start())

    kv_gather.forward()
    kv_gather.finish()

    def key_of(j, h):
        return kv_all[pl.ds(pl.multiple_of(j * tok, tok), tok), h * HD:(h + 1) * HD]

    def value_of(j, h):
        return kv_all[pl.ds(pl.multiple_of(j * tok, tok), tok), cols + h * HD:cols + (h + 1) * HD]

    deltas, inverses = [], []
    for h in range(heads):
        m_acc[...] = jnp.full(m_acc.shape, NEG, F32)
        l_acc[...] = jnp.zeros(l_acc.shape, F32)
        o_acc[...] = jnp.zeros(o_acc.shape, F32)

        def score(j):
            sc = dot_nt(q_st[h], key_of(j, h)) * scale
            row = lax.broadcasted_iota(jnp.int32, (m_rows, tok), 0) % tok
            col = lax.broadcasted_iota(jnp.int32, (m_rows, tok), 1)
            sc = jnp.where(col + j * tok <= row + s * tok, sc, NEG)
            s_scr[h * n + j] = sc
            m_acc[...] = jnp.maximum(m_acc[...], sc)

        loop(0, s + 1, score)
        top = jnp.max(m_acc[...], axis=1, keepdims=True)

        def weigh(j):
            e = jnp.exp(s_scr[h * n + j] - top)
            s_scr[h * n + j] = e
            l_acc[...] += e
            o_acc[...] += dot_nn(e.astype(BF16), value_of(j, h))

        loop(0, s + 1, weigh)
        inverse = 1.0 / jnp.sum(l_acc[...], axis=1, keepdims=True)
        out = o_acc[...] * inverse
        delta = jnp.sum(g_st[h].astype(F32) * out, axis=1, keepdims=True)
        for g in range(group):
            c = (h * group + g) * HD
            ao_ref[:, c:c + HD] = out[g * tok:(g + 1) * tok].astype(BF16)
        deltas.append(delta)
        inverses.append(inverse)

    if exchange:
        loop(1, n, x_arrived)
        loop(1, nf, lambda d: xf_copy(d).start())

    dq_acc[...] = jnp.zeros(dq_acc.shape, F32)

    def backward(j, h):
        p = s_scr[h * n + j] * inverses[h]
        dp = dot_nt(g_st[h], value_of(j, h))
        ds = (p * (dp - deltas[h])).astype(BF16)
        dv = dot_tn(p.astype(BF16), g_st[h])
        dk = dot_tn(ds, q_st[h])
        dq_acc[h] += dot_nn(ds, key_of(j, h))
        return dk, dv

    def rs_copy(j):
        return copy(rs_send.at[j], rs_recv.at[s], rs_s.at[j], rs_r.at[s], (j, f))

    def give(j):
        for h in range(heads):
            dk, dv = backward(j, h)
            rs_send[j, :, h * HD:(h + 1) * HD] = dk.astype(BF16)
            rs_send[j, :, cols + h * HD:cols + (h + 1) * HD] = dv.astype(BF16)
        rs_copy(j).start()

    loop(0, s, give)
    for h in range(heads):
        dk, dv = backward(s, h)
        own_dkv[:, h * HD:(h + 1) * HD] = dk
        own_dkv[:, cols + h * HD:cols + (h + 1) * HD] = dv
        for g in range(group):
            c = (h * group + g) * HD
            gq_ref[:, c:c + HD] = (dq_acc[h, g * tok:(g + 1) * tok] * scale).astype(BF16)

    def take(j):
        copy(rs_send.at[0], rs_recv.at[j], rs_s.at[0], rs_r.at[j], (mate, f)).wait_recv()
        own_dkv[...] += rs_recv[j].astype(F32)

    loop(s + 1, n, take)
    for h in range(heads):
        lin = own_dkv[:, h * HD:(h + 1) * HD] * scale
        turned = lin * cos_scr[...] - pltpu.roll(lin, HD // 2, 1) * sin_scr[...]
        dkv_all[own_rows, h * HD:(h + 1) * HD] = turned.astype(BF16)
    dkv_all[own_rows, cols:] = own_dkv[:, cols:].astype(BF16)
    dkv_gather.start()

    def input_term(b):
        at = pl.ds(pl.multiple_of(b * width, width), width)
        return (dot_nt(dkv_all[own_rows, :cols], wk_all[at, :])
                + dot_nt(dkv_all[own_rows, cols:], wv_all[at, :]))

    cores = 2 if nf % 2 == 0 else 1
    chips = nf // cores
    chip = f // cores
    core = f % cores
    twin = chip * cores + (cores - 1 - core)

    def gi_twin(o):
        return copy(gi_send.at[o], gi_recv.at[o], gi_s.at[o], gi_r.at[o], (s, twin))

    def gi_far(d):
        return copy(gi_send.at[chips + d], gi_recv.at[chips + chip], gi_s.at[chips + d],
                    gi_r.at[chips + chip], (s, (chip + d) % chips * cores + core))

    def twin_term(d):
        o = (chip + d) % chips
        gi_send[o] = input_term(o * cores + 1 - core).astype(BF16)
        gi_twin(o).start()

    def own_term(d):
        o = (chip + d) % chips
        gi_own[o] = input_term(o * cores + core)

    def join(d):
        o = (chip + d) % chips
        gi_twin(o).wait_recv()
        gi_own[o] += gi_recv[o].astype(F32)

    def far_term(d):
        if cores == 2:
            join(d)
        gi_send[chips + d] = gi_own[(chip + d) % chips].astype(BF16)
        gi_far(d).start()

    if cores == 2:
        loop(1, chips + 1, twin_term)
    loop(1, chips + 1, own_term)
    loop(1, chips, far_term)
    if cores == 2:
        join(0)
    if exchange:
        loop(1, nf, xf_arrived)
    dkv_gather.forward()
    dkv_gather.finish()

    total_tok = n * tok
    step = min(total_tok, 1024)
    for i in range(nf if exchange else 1):
        grad = None
        for at in range(0, total_tok, step):
            left = xt[i, at:at + step, :] if exchange else xt_in[at:at + step, :]
            term = dot_tn(left, dkv_all[at:at + step, :])
            grad = term if grad is None else grad + term
        count = grad.shape[0]
        gwk_ref[i * count:(i + 1) * count, :] = grad[:, :cols]
        gwv_ref[i * count:(i + 1) * count, :] = grad[:, cols:]

    def gi_take(d):
        b = (chip + d) % chips
        copy(gi_send.at[chips + d], gi_recv.at[chips + b], gi_s.at[chips + d],
             gi_r.at[chips + b], (s, b * cores + core)).wait_recv()
        gi_own[chip] += gi_recv[chips + b].astype(F32)

    loop(1, chips, gi_take)
    gi_ref[...] = gi_own[chip].astype(BF16)

    for gather in (wk_gather, wv_gather, kv_gather, dkv_gather):
        gather.drain()
    if exchange:
        loop(1, n, lambda d: x_copy(d).wait_send())
        loop(1, nf, lambda d: xf_copy(d).wait_send())
    loop(0, s, lambda j: rs_copy(j).wait_send())
    if cores == 2:
        loop(0, chips, lambda o: gi_twin(o).wait_send())
    loop(1, chips, lambda d: gi_far(d).wait_send())


def publish(*refs):
    count = len(refs) // 2
    sems = refs[-1]
    moves = [pltpu.make_async_copy(refs[i], refs[count + i], sems.at[i]) for i in range(count)]
    for move in moves:
        move.start()
    for move in moves:
        move.wait()


def body(n, nf, queries, layer_input, w_key, w_value, grad_out):
    tok, depth = layer_input.shape
    rows, cols = w_key.shape
    heads = cols // HD
    group = queries.shape[1] // cols
    m_rows = group * tok
    part = rows // nf
    exchange = part % 128 == 0
    half = HD // 2
    freq = np.float32(ROPE_BASE) ** (-(np.arange(half, dtype=np.float32) * np.float32(2.0 / HD)))
    freq = jnp.asarray(np.concatenate([freq, freq])[None, :], F32)
    operands = [queries, layer_input, w_key, w_value, grad_out, freq]
    if not exchange:
        operands.append(
            lax.all_to_all(layer_input, "seq", split_axis=1, concat_axis=0, tiled=True))
    width = depth // nf
    x_rows = n * tok if exchange else 16
    x_cols = part if exchange else 128
    vmem = pltpu.VMEM
    dma = pltpu.SemaphoreType.DMA
    scratch = [
        vmem((depth, cols), BF16), vmem((depth, cols), BF16),
        vmem((n * tok, 2 * cols), BF16), vmem((n * tok, 2 * cols), BF16),
        vmem((nf, x_rows, x_cols), BF16),
        vmem((heads, m_rows, HD), BF16), vmem((heads, m_rows, HD), BF16),
        vmem((m_rows, HD), F32), vmem((heads, m_rows, HD), F32),
        vmem((m_rows, tok), F32), vmem((m_rows, tok), F32),
        vmem((heads * n, m_rows, tok), F32),
        vmem((n, tok, 2 * cols), BF16), vmem((n, tok, 2 * cols), BF16),
        vmem((tok, 2 * cols), F32),
        vmem((tok, HD), F32), vmem((tok, HD), F32),
        vmem((2 * nf, tok, width), BF16), vmem((2 * nf, tok, width), BF16),
        vmem((nf, tok, width), F32),
    ]
    for _ in range(4):
        scratch += [dma((3 * n,)), dma((n,))]
    scratch += [dma((n,)), dma((n,)), dma((nf,)), dma((nf,))]
    scratch += [dma((n,)), dma((n,)), dma((2 * nf,)), dma((2 * nf,))]
    scratch += [vmem(queries.shape, BF16), vmem((tok, depth), BF16), vmem(queries.shape, BF16),
                dma((5,))]
    out_shape = [
        jax.ShapeDtypeStruct(queries.shape, BF16),
        jax.ShapeDtypeStruct(queries.shape, BF16),
        jax.ShapeDtypeStruct((tok, width), BF16),
        jax.ShapeDtypeStruct((rows, cols), F32),
        jax.ShapeDtypeStruct((rows, cols), F32),
    ]
    spec = pl.BlockSpec(memory_space=pltpu.VMEM)
    whole = pl.BlockSpec(memory_space=pl.ANY)
    results = pl.pallas_call(
        functools.partial(kernel, (n, nf, exchange)),
        out_shape=[pltpu.VMEM(o.shape, o.dtype) for o in out_shape],
        in_specs=[whole] * 5 + [spec] * (len(operands) - 5),
        out_specs=[spec] * len(out_shape),
        scratch_shapes=scratch,
        compiler_params=pltpu.CompilerParams(
            collective_id=0, has_side_effects=True, vmem_limit_bytes=60 * 1024 * 1024),
    )(*operands)
    return tuple(pl.pallas_call(
        publish,
        out_shape=out_shape,
        in_specs=[spec] * len(out_shape),
        out_specs=[whole] * len(out_shape),
        scratch_shapes=[dma((len(out_shape),))],
        compiler_params=pltpu.CompilerParams(vmem_limit_bytes=8 * 1024 * 1024),
    )(*results))


def solution(mesh):
    placed = (
        P("seq", "fsdp"),
        P("seq", None),
        P("seq", "fsdp"),
        P("seq", "fsdp"),
        P("seq", "fsdp"),
    )
    return jax.shard_map(
        functools.partial(body, mesh.shape["seq"], mesh.shape["fsdp"]),
        mesh=mesh,
        in_specs=placed,
        out_specs=(P("seq", "fsdp"),) * 5,
        check_vma=False,
    )
```

```python
import functools

import jax
import jax.numpy as jnp
import numpy as np
from jax import lax
from jax.experimental import pallas as pl
from jax.experimental.pallas import tpu as pltpu
from jax.sharding import PartitionSpec as P

HD = 128
ROPE_BASE = 500000.0
NEG = -1e30
MESH = pl.DeviceIdType.MESH
F32 = jnp.float32
BF16 = jnp.bfloat16


def loop(low, high, step):
    def run(i, carry):
        step(i)
        return carry

    lax.fori_loop(low, high, run, 0)


def dot_nn(a, b):
    return lax.dot_general(a, b, (((1,), (0,)), ((), ())), preferred_element_type=F32)


def dot_nt(a, b):
    return lax.dot_general(a, b, (((1,), (1,)), ((), ())), preferred_element_type=F32)


def dot_tn(a, b):
    return lax.dot_general(a, b, (((0,), (0,)), ((), ())), preferred_element_type=F32)


def kernel(cfg, *refs):
    n, nf, exchange = cfg
    q_hbm, x_hbm, wk_ref, wv_ref, g_hbm, freq_ref = refs[:6]
    refs = refs[6:]
    if not exchange:
        xt_in = refs[0]
        refs = refs[1:]
    ao_ref, gq_ref, gi_ref, gwk_ref, gwv_ref = refs[:5]
    (wk_all, wv_all, kv_all, dkv_all, xt, q_st, g_st, o_acc, dq_acc, m_acc, l_acc, s_scr,
     rs_send, rs_recv, own_dkv, cos_scr, sin_scr, gi_send, gi_recv, gi_own,
     wk_s, wk_r, wv_s, wv_r, kv_s, kv_r, dkv_s, dkv_r, x_s, x_r, xf_s, xf_r,
     rs_s, rs_r, gi_s, gi_r, q_ref, x_ref, g_ref, in_s) = refs[5:]
    tok = x_ref.shape[0]
    rows, cols = wk_ref.shape
    heads = cols // HD
    group = q_ref.shape[1] // cols
    m_rows = group * tok
    part = rows // nf
    width = gi_ref.shape[1]
    scale = HD ** (-0.5)
    s = lax.axis_index("seq")
    f = lax.axis_index("fsdp")
    inner = 2 if n % 2 == 0 else 1
    outer = n // inner
    z = s // inner
    y = s % inner
    mate = z * inner + (inner - 1 - y)

    def copy(src, dst, send, recv, dev):
        return pltpu.make_async_remote_copy(
            src_ref=src, dst_ref=dst, send_sem=send, recv_sem=recv, device_id=dev,
            device_id_type=MESH,
        )

    barrier = pltpu.get_barrier_semaphore()

    def greet_seq(d):
        pl.semaphore_signal(
            barrier, inc=1, device_id=((s + d) % n, f), device_id_type=MESH)

    def greet_fsdp(d):
        pl.semaphore_signal(
            barrier, inc=1, device_id=(s, (f + d) % nf), device_id_type=MESH)

    loop(1, n, greet_seq)
    loop(1, nf, greet_fsdp)
    mine = pl.ds(pl.multiple_of(s * rows, rows), rows)
    loads = [
        pltpu.make_async_copy(src, dst, in_s.at[i])
        for i, (src, dst) in enumerate((
            (wk_ref, wk_all.at[mine]), (wv_ref, wv_all.at[mine]),
            (x_hbm, x_ref), (q_hbm, q_ref), (g_hbm, g_ref)))
    ]
    for load in loads:
        load.start()
    pl.semaphore_wait(barrier, n + nf - 2)

    class Gather:
        def __init__(self, own, slot, send, recv, causal=False):
            self.own, self.slot, self.send, self.recv = own, slot, send, recv
            self.give_to = outer - z if causal else outer
            self.take_from = z + 1 if causal else outer

        def outgoing(self, d):
            return copy(self.own, self.slot(s), self.send.at[d], self.recv.at[s],
                        ((z + d) % outer * inner + y, f))

        def to_mate(self):
            return copy(self.own, self.slot(s), self.send.at[0], self.recv.at[s], (mate, f))

        def arrived(self, b):
            copy(self.own, self.slot(b), self.send.at[0], self.recv.at[b], (mate, f)).wait_recv()

        def pass_on(self, d):
            b = (z - d + outer) % outer * inner + y
            return copy(self.slot(b), self.slot(b), self.send.at[outer + d], self.recv.at[b],
                        (mate, f))

        def start(self):
            if inner == 2:
                self.to_mate().start()
            loop(1, self.give_to, lambda d: self.outgoing(d).start())

        def forward(self):
            def step(d):
                self.arrived((z - d + outer) % outer * inner + y)
                if inner == 2:
                    self.pass_on(d).start()

            loop(1, self.take_from, step)

        def finish(self):
            if inner == 2:
                loop(0, self.take_from, lambda d: self.arrived(
                    (z - d + outer) % outer * inner + (inner - 1 - y)))

        def drain(self):
            if inner == 2:
                self.to_mate().wait_send()
            loop(1, self.give_to, lambda d: self.outgoing(d).wait_send())
            if inner == 2:
                loop(1, self.take_from, lambda d: self.pass_on(d).wait_send())

    class Line(Gather):
        def hop(self, b, way):
            ref = self.slot(b)
            dev = (z + 1) * inner + y if way == 0 else (z - 1) * inner + y if way == 1 else mate
            return copy(ref, ref, self.send.at[way * n + b], self.recv.at[b], (dev, f))

        def first(self, way):
            dev = (z + 1) * inner + y if way == 0 else (z - 1) * inner + y if way == 1 else mate
            return copy(self.own, self.slot(s), self.send.at[way * n + s], self.recv.at[s],
                        (dev, f))

        def start(self):
            pl.when(z < outer - 1)(lambda: self.first(0).start())
            pl.when(z > 0)(lambda: self.first(1).start())
            if inner == 2:
                self.first(2).start()

        def relay(self, d, act):
            below = (z - d) * inner + y
            above = (z + d) * inner + y

            @pl.when(z >= d)
            def _():
                if act == "start":
                    self.arrived(below)
                for way in (0, 2) if inner == 2 else (0,):
                    def go(way=way):
                        getattr(self.hop(below, way), act)()
                    if way == 0:
                        pl.when(z < outer - 1)(go)
                    else:
                        go()

            @pl.when(z + d < outer)
            def _():
                if act == "start":
                    self.arrived(above)
                for way in (1, 2) if inner == 2 else (1,):
                    def go(way=way):
                        getattr(self.hop(above, way), act)()
                    if way == 1:
                        pl.when(z > 0)(go)
                    else:
                        go()

        def drain(self):
            pl.when(z < outer - 1)(lambda: self.first(0).wait_send())
            pl.when(z > 0)(lambda: self.first(1).wait_send())
            if inner == 2:
                self.first(2).wait_send()
            loop(1, outer, lambda d: self.relay(d, "wait_send"))

    def row_slot(ref, size):
        return lambda b: ref.at[pl.ds(pl.multiple_of(b * size, size), size)]

    wk_slot, wv_slot = row_slot(wk_all, rows), row_slot(wv_all, rows)
    wk_gather = Line(wk_slot(s), wk_slot, wk_s, wk_r)
    wv_gather = Line(wv_slot(s), wv_slot, wv_s, wv_r)
    kv_slot = row_slot(kv_all, tok)
    kv_gather = Gather(kv_slot(s), kv_slot, kv_s, kv_r, causal=True)
    dkv_slot = row_slot(dkv_all, tok)
    dkv_gather = Gather(dkv_slot(s), dkv_slot, dkv_s, dkv_r)

    loads[0].wait()
    wk_gather.start()
    loads[1].wait()
    wv_gather.start()
    for load in loads[2:]:
        load.wait()

    if exchange:
        def x_src(b):
            return x_ref.at[:, pl.ds(pl.multiple_of(b * rows + f * part, part), part)]

        def x_copy(d):
            b = (s + d) % n
            return copy(x_src(b), xt.at[f, pl.ds(pl.multiple_of(s * tok, tok), tok)],
                        x_s.at[d], x_r.at[s], (b, f))

        def x_arrived(d):
            b = (s + d) % n
            copy(x_src(b), xt.at[f, pl.ds(pl.multiple_of(b * tok, tok), tok)],
                 x_s.at[d], x_r.at[b], (b, f)).wait_recv()

        def xf_copy(d):
            return copy(xt.at[f], xt.at[f], xf_s.at[d], xf_r.at[f], (s, (f + d) % nf))

        def xf_arrived(d):
            b = (f + d) % nf
            copy(xt.at[f], xt.at[b], xf_s.at[d], xf_r.at[b], (s, b)).wait_recv()

        xt[f, pl.ds(pl.multiple_of(s * tok, tok), tok), :] = x_ref[
            :, pl.ds(pl.multiple_of(s * rows + f * part, part), part)]

    for h in range(heads):
        for g in range(group):
            c = (h * group + g) * HD
            q_st[h, g * tok:(g + 1) * tok, :] = q_ref[:, c:c + HD]
            g_st[h, g * tok:(g + 1) * tok, :] = g_ref[:, c:c + HD]
    lane = lax.broadcasted_iota(jnp.int32, (tok, HD), 1)
    position = (s * tok + lax.broadcasted_iota(jnp.int32, (tok, HD), 0)).astype(F32)
    angle = position * freq_ref[...]
    cos_scr[...] = jnp.cos(angle)
    sin_scr[...] = jnp.where(lane < HD // 2, -jnp.sin(angle), jnp.sin(angle))

    def relay_weights(d):
        wk_gather.relay(d, "start")
        wv_gather.relay(d, "start")

    loop(1, outer, relay_weights)
    wk_gather.finish()
    wv_gather.finish()

    key_lin = dot_nn(x_ref[...], wk_all[...])
    value_lin = dot_nn(x_ref[...], wv_all[...])
    own_rows = pl.ds(pl.multiple_of(s * tok, tok), tok)
    for h in range(heads):
        lin = key_lin[:, h * HD:(h + 1) * HD]
        turned = lin * cos_scr[...] + pltpu.roll(lin, HD // 2, 1) * sin_scr[...]
        kv_all[own_rows, h * HD:(h + 1) * HD] = turned.astype(BF16)
    kv_all[own_rows, cols:] = value_lin.astype(BF16)
    kv_gather.start()

    if exchange:
        loop(1, n, lambda d: x_copy(d).start())

    kv_gather.forward()
    kv_gather.finish()

    def key_of(j, h):
        return kv_all[pl.ds(pl.multiple_of(j * tok, tok), tok), h * HD:(h + 1) * HD]

    def value_of(j, h):
        return kv_all[pl.ds(pl.multiple_of(j * tok, tok), tok), cols + h * HD:cols + (h + 1) * HD]

    deltas, inverses = [], []
    for h in range(heads):
        m_acc[...] = jnp.full(m_acc.shape, NEG, F32)
        l_acc[...] = jnp.zeros(l_acc.shape, F32)
        o_acc[...] = jnp.zeros(o_acc.shape, F32)

        def score(j):
            sc = dot_nt(q_st[h], key_of(j, h)) * scale
            row = lax.broadcasted_iota(jnp.int32, (m_rows, tok), 0) % tok
            col = lax.broadcasted_iota(jnp.int32, (m_rows, tok), 1)
            sc = jnp.where(col + j * tok <= row + s * tok, sc, NEG)
            s_scr[h * n + j] = sc
            m_acc[...] = jnp.maximum(m_acc[...], sc)

        loop(0, s + 1, score)
        top = jnp.max(m_acc[...], axis=1, keepdims=True)

        def weigh(j):
            e = jnp.exp(s_scr[h * n + j] - top)
            s_scr[h * n + j] = e
            l_acc[...] += e
            o_acc[...] += dot_nn(e.astype(BF16), value_of(j, h))

        loop(0, s + 1, weigh)
        inverse = 1.0 / jnp.sum(l_acc[...], axis=1, keepdims=True)
        out = o_acc[...] * inverse
        delta = jnp.sum(g_st[h].astype(F32) * out, axis=1, keepdims=True)
        for g in range(group):
            c = (h * group + g) * HD
            ao_ref[:, c:c + HD] = out[g * tok:(g + 1) * tok].astype(BF16)
        deltas.append(delta)
        inverses.append(inverse)

    if exchange:
        loop(1, n, x_arrived)
        loop(1, nf, lambda d: xf_copy(d).start())

    dq_acc[...] = jnp.zeros(dq_acc.shape, F32)

    def backward(j, h):
        p = s_scr[h * n + j] * inverses[h]
        dp = dot_nt(g_st[h], value_of(j, h))
        ds = (p * (dp - deltas[h])).astype(BF16)
        dv = dot_tn(p.astype(BF16), g_st[h])
        dk = dot_tn(ds, q_st[h])
        dq_acc[h] += dot_nn(ds, key_of(j, h))
        return dk, dv

    def rs_copy(j):
        return copy(rs_send.at[j], rs_recv.at[s], rs_s.at[j], rs_r.at[s], (j, f))

    def give(j):
        for h in range(heads):
            dk, dv = backward(j, h)
            rs_send[j, :, h * HD:(h + 1) * HD] = dk.astype(BF16)
            rs_send[j, :, cols + h * HD:cols + (h + 1) * HD] = dv.astype(BF16)
        rs_copy(j).start()

    loop(0, s, give)
    for h in range(heads):
        dk, dv = backward(s, h)
        own_dkv[:, h * HD:(h + 1) * HD] = dk
        own_dkv[:, cols + h * HD:cols + (h + 1) * HD] = dv
        for g in range(group):
            c = (h * group + g) * HD
            gq_ref[:, c:c + HD] = (dq_acc[h, g * tok:(g + 1) * tok] * scale).astype(BF16)

    def take(j):
        copy(rs_send.at[0], rs_recv.at[j], rs_s.at[0], rs_r.at[j], (mate, f)).wait_recv()
        own_dkv[...] += rs_recv[j].astype(F32)

    loop(s + 1, n, take)
    for h in range(heads):
        lin = own_dkv[:, h * HD:(h + 1) * HD] * scale
        turned = lin * cos_scr[...] - pltpu.roll(lin, HD // 2, 1) * sin_scr[...]
        dkv_all[own_rows, h * HD:(h + 1) * HD] = turned.astype(BF16)
    dkv_all[own_rows, cols:] = own_dkv[:, cols:].astype(BF16)
    dkv_gather.start()

    def input_term(b):
        at = pl.ds(pl.multiple_of(b * width, width), width)
        return (dot_nt(dkv_all[own_rows, :cols], wk_all[at, :])
                + dot_nt(dkv_all[own_rows, cols:], wv_all[at, :]))

    cores = 2 if nf % 2 == 0 else 1
    chips = nf // cores
    chip = f // cores
    core = f % cores
    twin = chip * cores + (cores - 1 - core)

    def gi_twin(o):
        return copy(gi_send.at[o], gi_recv.at[o], gi_s.at[o], gi_r.at[o], (s, twin))

    def gi_far(d):
        return copy(gi_send.at[chips + d], gi_recv.at[chips + chip], gi_s.at[chips + d],
                    gi_r.at[chips + chip], (s, (chip + d) % chips * cores + core))

    def twin_term(d):
        o = (chip + d) % chips
        gi_send[o] = input_term(o * cores + 1 - core).astype(BF16)
        gi_twin(o).start()

    def own_term(d):
        o = (chip + d) % chips
        gi_own[o] = input_term(o * cores + core)

    def join(d):
        o = (chip + d) % chips
        gi_twin(o).wait_recv()
        gi_own[o] += gi_recv[o].astype(F32)

    def far_term(d):
        if cores == 2:
            join(d)
        gi_send[chips + d] = gi_own[(chip + d) % chips].astype(BF16)
        gi_far(d).start()

    if cores == 2:
        loop(1, chips + 1, twin_term)
    loop(1, chips + 1, own_term)
    loop(1, chips, far_term)
    if cores == 2:
        join(0)
    dkv_gather.forward()
    dkv_gather.finish()
    if exchange:
        loop(1, nf, xf_arrived)

    total_tok = n * tok
    step = min(total_tok, 1024)
    for i in range(nf if exchange else 1):
        grad = None
        for at in range(0, total_tok, step):
            left = xt[i, at:at + step, :] if exchange else xt_in[at:at + step, :]
            term = dot_tn(left, dkv_all[at:at + step, :])
            grad = term if grad is None else grad + term
        count = grad.shape[0]
        gwk_ref[i * count:(i + 1) * count, :] = grad[:, :cols]
        gwv_ref[i * count:(i + 1) * count, :] = grad[:, cols:]

    def gi_take(d):
        b = (chip + d) % chips
        copy(gi_send.at[chips + d], gi_recv.at[chips + b], gi_s.at[chips + d],
             gi_r.at[chips + b], (s, b * cores + core)).wait_recv()
        gi_own[chip] += gi_recv[chips + b].astype(F32)

    loop(1, chips, gi_take)
    gi_ref[...] = gi_own[chip].astype(BF16)

    for gather in (wk_gather, wv_gather, kv_gather, dkv_gather):
        gather.drain()
    if exchange:
        loop(1, n, lambda d: x_copy(d).wait_send())
        loop(1, nf, lambda d: xf_copy(d).wait_send())
    loop(0, s, lambda j: rs_copy(j).wait_send())
    if cores == 2:
        loop(0, chips, lambda o: gi_twin(o).wait_send())
    loop(1, chips, lambda d: gi_far(d).wait_send())


def publish(*refs):
    count = len(refs) // 2
    sems = refs[-1]
    moves = [pltpu.make_async_copy(refs[i], refs[count + i], sems.at[i]) for i in range(count)]
    for move in moves:
        move.start()
    for move in moves:
        move.wait()


def body(n, nf, queries, layer_input, w_key, w_value, grad_out):
    tok, depth = layer_input.shape
    rows, cols = w_key.shape
    heads = cols // HD
    group = queries.shape[1] // cols
    m_rows = group * tok
    part = rows // nf
    exchange = part % 128 == 0
    half = HD // 2
    freq = np.float32(ROPE_BASE) ** (-(np.arange(half, dtype=np.float32) * np.float32(2.0 / HD)))
    freq = jnp.asarray(np.concatenate([freq, freq])[None, :], F32)
    operands = [queries, layer_input, w_key, w_value, grad_out, freq]
    if not exchange:
        operands.append(
            lax.all_to_all(layer_input, "seq", split_axis=1, concat_axis=0, tiled=True))
    width = depth // nf
    x_rows = n * tok if exchange else 16
    x_cols = part if exchange else 128
    vmem = pltpu.VMEM
    dma = pltpu.SemaphoreType.DMA
    scratch = [
        vmem((depth, cols), BF16), vmem((depth, cols), BF16),
        vmem((n * tok, 2 * cols), BF16), vmem((n * tok, 2 * cols), BF16),
        vmem((nf, x_rows, x_cols), BF16),
        vmem((heads, m_rows, HD), BF16), vmem((heads, m_rows, HD), BF16),
        vmem((m_rows, HD), F32), vmem((heads, m_rows, HD), F32),
        vmem((m_rows, tok), F32), vmem((m_rows, tok), F32),
        vmem((heads * n, m_rows, tok), F32),
        vmem((n, tok, 2 * cols), BF16), vmem((n, tok, 2 * cols), BF16),
        vmem((tok, 2 * cols), F32),
        vmem((tok, HD), F32), vmem((tok, HD), F32),
        vmem((2 * nf, tok, width), BF16), vmem((2 * nf, tok, width), BF16),
        vmem((nf, tok, width), F32),
    ]
    for _ in range(4):
        scratch += [dma((3 * n,)), dma((n,))]
    scratch += [dma((n,)), dma((n,)), dma((nf,)), dma((nf,))]
    scratch += [dma((n,)), dma((n,)), dma((2 * nf,)), dma((2 * nf,))]
    scratch += [vmem(queries.shape, BF16), vmem((tok, depth), BF16), vmem(queries.shape, BF16),
                dma((5,))]
    out_shape = [
        jax.ShapeDtypeStruct(queries.shape, BF16),
        jax.ShapeDtypeStruct(queries.shape, BF16),
        jax.ShapeDtypeStruct((tok, width), BF16),
        jax.ShapeDtypeStruct((rows, cols), F32),
        jax.ShapeDtypeStruct((rows, cols), F32),
    ]
    spec = pl.BlockSpec(memory_space=pltpu.VMEM)
    whole = pl.BlockSpec(memory_space=pl.ANY)
    results = pl.pallas_call(
        functools.partial(kernel, (n, nf, exchange)),
        out_shape=[pltpu.VMEM(o.shape, o.dtype) for o in out_shape],
        in_specs=[whole] * 5 + [spec] * (len(operands) - 5),
        out_specs=[spec] * len(out_shape),
        scratch_shapes=scratch,
        compiler_params=pltpu.CompilerParams(
            collective_id=0, has_side_effects=True, vmem_limit_bytes=60 * 1024 * 1024),
    )(*operands)
    return tuple(pl.pallas_call(
        publish,
        out_shape=out_shape,
        in_specs=[spec] * len(out_shape),
        out_specs=[whole] * len(out_shape),
        scratch_shapes=[dma((len(out_shape),))],
        compiler_params=pltpu.CompilerParams(vmem_limit_bytes=8 * 1024 * 1024),
    )(*results))


def solution(mesh):
    placed = (
        P("seq", "fsdp"),
        P("seq", None),
        P("seq", "fsdp"),
        P("seq", "fsdp"),
        P("seq", "fsdp"),
    )
    return jax.shard_map(
        functools.partial(body, mesh.shape["seq"], mesh.shape["fsdp"]),
        mesh=mesh,
        in_specs=placed,
        out_specs=(P("seq", "fsdp"),) * 5,
        check_vma=False,
    )
```
